8 devices in a mesh: rep: 1 (over z), head: 2 (over y), seq: 4 (over x, core).
Axes of the slice: x: 2, y: 2, z: 1, core: 2. Of those that a mesh axis runs over, the one named last changes fastest.
Arguments:
- tokens: bfloat16 [64, 4096], P('rep')
- w_query: bfloat16 [4096, 4096], replicated
- w_key: bfloat16 [4096, 1024], replicated
- w_value: bfloat16 [4096, 1024], replicated
- w_out: bfloat16 [4096, 4096], P(('head', 'seq'))
- k_cache: bfloat16 [64, 1024, 8, 128], P('rep', 'seq', 'head')
- v_cache: bfloat16 [64, 1024, 8, 128], P('rep', 'seq', 'head')
- positions: int32 [64], P('rep')
Outputs:
- output 1: bfloat16 [64, 4096], P('rep')
- output 2: bfloat16 [64, 1024, 8, 128], P('rep', 'seq', 'head')
- output 3: bfloat16 [64, 1024, 8, 128], P('rep', 'seq', 'head')
All inputs are finite; a program needn't handle non-finite values.
Results may differ from the reference program's by a relative error of at most 0.00655092.
Values are sent between devices in bfloat16 or wider.
A program may use at most 1 GiB of HBM per device.

```python
import math
import jax
import jax.numpy as jnp
from jax import lax

BATCH = 64
D_MODEL = 4096
N_HEADS = 32
N_KV = 8
HEAD_DIM = 128
SHARD_LEN = 256
SEQ_LEN = 1024
KEY_SCALE = math.sqrt(math.log(SHARD_LEN / 16))


def setup_inputs(seed: int = 0, part: int = 0) -> dict:
    base_key = jax.random.key(seed)
    part_key = jax.random.fold_in(base_key, part)
    weight_keys = jax.random.split(base_key, 4)
    part_keys = jax.random.split(part_key, 4)
    tokens = jax.random.normal(part_keys[0], (BATCH, D_MODEL), jnp.float32)
    w_query = jax.random.normal(weight_keys[0], (D_MODEL, N_HEADS * HEAD_DIM), jnp.float32) * D_MODEL ** -0.5
    w_key = jax.random.normal(weight_keys[1], (D_MODEL, N_KV * HEAD_DIM), jnp.float32) * (KEY_SCALE * D_MODEL ** -0.5)
    w_value = jax.random.normal(weight_keys[2], (D_MODEL, N_KV * HEAD_DIM), jnp.float32) * D_MODEL ** -0.5
    w_out = jax.random.normal(weight_keys[3], (N_HEADS * HEAD_DIM, D_MODEL), jnp.float32) * (N_HEADS * HEAD_DIM) ** -0.5
    k_cache = jax.random.normal(part_keys[1], (BATCH, SEQ_LEN, N_KV, HEAD_DIM), jnp.float32) * KEY_SCALE
    v_cache = jax.random.normal(part_keys[2], (BATCH, SEQ_LEN, N_KV, HEAD_DIM), jnp.float32)
    positions = jax.random.randint(part_keys[3], (BATCH,), 0, SEQ_LEN, jnp.int32)
    positions = positions.at[0].set(SEQ_LEN - 1)
    return {
        'tokens': tokens.astype(jnp.bfloat16),
        'w_query': w_query.astype(jnp.bfloat16),
        'w_key': w_key.astype(jnp.bfloat16),
        'w_value': w_value.astype(jnp.bfloat16),
        'w_out': w_out.astype(jnp.bfloat16),
        'k_cache': k_cache.astype(jnp.bfloat16),
        'v_cache': v_cache.astype(jnp.bfloat16),
        'positions': positions,
    }


def reference(tokens, w_query, w_key, w_value, w_out, k_cache, v_cache, positions):
    groups = N_HEADS // N_KV
    query = jnp.dot(tokens, w_query, preferred_element_type=jnp.float32).astype(jnp.bfloat16)
    new_key = jnp.dot(tokens, w_key, preferred_element_type=jnp.float32).astype(jnp.bfloat16)
    new_value = jnp.dot(tokens, w_value, preferred_element_type=jnp.float32).astype(jnp.bfloat16)
    query = query.reshape(BATCH, N_KV, groups, HEAD_DIM)
    new_key = new_key.reshape(BATCH, N_KV, HEAD_DIM)
    new_value = new_value.reshape(BATCH, N_KV, HEAD_DIM)
    slot_ids = jnp.arange(SEQ_LEN, dtype=jnp.int32)

    def one_row(row_inputs):
        q_row, key_row, value_row, k_rows, v_rows, pos_row = row_inputs
        is_slot = (slot_ids == pos_row)[:, None, None]
        k_new = jnp.where(is_slot, key_row[None], k_rows)
        v_new = jnp.where(is_slot, value_row[None], v_rows)
        scores = jnp.einsum('kgd,tkd->kgt', q_row.astype(jnp.float32), k_new.astype(jnp.float32)) * HEAD_DIM ** -0.5
        scores = jnp.where(slot_ids <= pos_row, scores, -jnp.inf)
        row_max = jnp.max(scores, axis=-1, keepdims=True)
        weights = jnp.exp(scores - row_max)
        row_sum = jnp.sum(weights, axis=-1, keepdims=True)
        mixed_sum = jnp.einsum('kgt,tkd->kgd', weights.astype(jnp.bfloat16).astype(jnp.float32), v_new.astype(jnp.float32))
        attn_row = (mixed_sum / row_sum).astype(jnp.bfloat16)
        return k_new, v_new, attn_row

    k_out, v_out, attn_rows = lax.map(one_row, (query, new_key, new_value, k_cache, v_cache, positions))
    attn_flat = attn_rows.reshape(BATCH, N_HEADS * HEAD_DIM)
    y_out = jnp.dot(attn_flat, w_out, preferred_element_type=jnp.float32).astype(jnp.bfloat16)
    return y_out, k_out, v_out
```

```python
import functools

import jax
import jax.numpy as jnp
from jax import lax
from jax.experimental import pallas as pl
from jax.experimental.pallas import tpu as pltpu
from jax.sharding import PartitionSpec as P

MESH = pl.DeviceIdType.MESH
BF16 = jnp.bfloat16
F32 = jnp.float32
MIB = 2 ** 20
GB = 8
D = 128
LOG2E = 1.4426950408889634


def attend_kernel(dims, pos_ref, x_ref, wq, wk, wv, kc, vc, ko, vo, mix_ref, st_ref,
                  k_vm, v_vm, w_vm, q_s, nk_s, nv_s, s_s, w_sem, k_sem, v_sem, ko_sem, vo_sem):
    kv, groups, shard, n_groups, slots = dims
    heads = kv * groups
    rows = shard * kv
    lanes = heads * GB
    head_i, seq_i = lax.axis_index("head"), lax.axis_index("seq")
    base = seq_i * shard
    cols = kv * D
    n_q = heads // kv

    def w_copy(c):
        if c < n_q:
            src, at = wq, head_i * (heads * D) + c * cols
        else:
            src, at = (wk, wv)[c - n_q], head_i * cols
        at = pl.multiple_of(at, cols)
        return pltpu.make_async_copy(src.at[:, pl.ds(at, cols)], w_vm.at[c % slots], w_sem.at[c % slots])

    def k_copy(g):
        at = pl.ds(g * GB, GB)
        return pltpu.make_async_copy(kc.at[at], k_vm.at[at], k_sem.at[g])

    def v_copy(g):
        at = pl.ds(g * GB, GB)
        return pltpu.make_async_copy(vc.at[at], v_vm.at[at], v_sem.at[g])

    def ko_copy(g):
        at = pl.ds(g * GB, GB)
        return pltpu.make_async_copy(k_vm.at[at], ko.at[at], ko_sem.at[g])

    def vo_copy(g):
        at = pl.ds(g * GB, GB)
        return pltpu.make_async_copy(v_vm.at[at], vo.at[at], vo_sem.at[g])

    n_w = n_q + 2
    ahead = 4
    for c in range(min(slots, n_w)):
        w_copy(c).start()
    issued = 0
    for c in range(n_w):
        w_copy(c).wait()
        r = jnp.dot(x_ref[...], w_vm[c % slots], preferred_element_type=F32)
        r = r.astype(BF16).astype(F32)
        for i in range(kv):
            part = r[:, i * D:(i + 1) * D]
            if c < n_q:
                q_s[c * kv + i] = part
            elif c == n_q:
                nk_s[i] = part
            else:
                nv_s[i] = part
        if c + slots < n_w:
            w_copy(c + slots).start()
        else:
            while issued < min(ahead, n_groups) and issued <= (c + slots - n_w + 1):
                k_copy(issued).start()
                v_copy(issued).start()
                issued += 1
    for g in range(issued, min(ahead, n_groups)):
        k_copy(g).start()
        v_copy(g).start()

    r16 = lax.broadcasted_iota(jnp.int32, (16, D), 0)

    def new_rows(src, b):
        out = jnp.broadcast_to(src[kv - 1, pl.ds(b, 1), :], (16, D))
        for j in range(kv - 1):
            out = jnp.where(r16 % kv == j, jnp.broadcast_to(src[j, pl.ds(b, 1), :], (16, D)), out)
        return out

    sub = lax.broadcasted_iota(jnp.int32, (8, lanes), 0)
    lane = lax.broadcasted_iota(jnp.int32, (8, lanes), 1)
    lane_d = lax.broadcasted_iota(jnp.int32, (D, lanes), 1)
    row_l = lax.broadcasted_iota(jnp.int32, (lanes, D), 0)
    per_tile = 8 // kv
    scale2 = (D ** -0.5) * LOG2E

    def group(g, carry):
        @pl.when(g + ahead < n_groups)
        def _():
            k_copy(g + ahead).start()
            v_copy(g + ahead).start()
        k_copy(g).wait()
        v_copy(g).wait()
        pos_row = jnp.zeros((8, lanes), jnp.int32)
        for i in range(GB):
            b = g * GB + i
            t = pos_ref[b] - base
            pos_row = jnp.where(lane % GB == i, t, pos_row)

            @pl.when(jnp.logical_and(t >= 0, t < shard))
            def _():
                at = pl.ds(pl.multiple_of((t // (16 // kv)) * 16, 16), 16)
                hit = r16 // kv == t % (16 // kv)
                k_vm[b, at, :] = jnp.where(hit, new_rows(nk_s, b), k_vm[b, at, :].astype(F32)).astype(BF16)
                v_vm[b, at, :] = jnp.where(hit, new_rows(nv_s, b), v_vm[b, at, :].astype(F32)).astype(BF16)
        ko_copy(g).start()
        vo_copy(g).start()

        q_t = q_s[:, pl.ds(pl.multiple_of(g * GB, GB), GB), :].reshape(lanes, D).T
        acc = None
        for p in range(GB // 2):
            keys = jnp.concatenate([k_vm[g * GB + 2 * p], k_vm[g * GB + 2 * p + 1]], axis=1)
            qs = jnp.concatenate([jnp.where(lane_d % GB == 2 * p, q_t, 0.0),
                                  jnp.where(lane_d % GB == 2 * p + 1, q_t, 0.0)], axis=0).astype(BF16)
            s = jnp.dot(keys, qs, preferred_element_type=F32)
            acc = s if acc is None else acc + s
        limit = jnp.where(sub % kv == lane // (groups * GB), pos_row - sub // kv, -1)
        tile_t = lax.broadcasted_iota(jnp.int32, (rows // 8, 8, lanes), 0) * per_tile
        s3 = jnp.where(limit[None] >= tile_t, acc.reshape(rows // 8, 8, lanes), -jnp.inf)
        s_s[...] = s3
        m = jnp.max(jnp.max(s3, axis=0), axis=0, keepdims=True)
        m_safe = jnp.where(m > -jnp.inf, m, 0.0)
        w3 = jnp.exp2((s_s[...] - m_safe[None]) * scale2)
        st_ref[pl.ds(g, 1), :] = m
        st_ref[pl.ds(n_groups + g, 1), :] = jnp.sum(jnp.sum(w3, axis=0), axis=0, keepdims=True)
        w_t = w3.reshape(rows, lanes).astype(BF16).T
        mix = jnp.zeros((lanes, D), F32)
        for p in range(GB // 2):
            vals = jnp.concatenate([v_vm[g * GB + 2 * p], v_vm[g * GB + 2 * p + 1]], axis=1)
            o = jnp.dot(w_t, vals, preferred_element_type=F32)
            mix = jnp.where(row_l % GB == 2 * p, o[:, :D], mix)
            mix = jnp.where(row_l % GB == 2 * p + 1, o[:, D:], mix)
        mix_ref[:, pl.ds(pl.multiple_of(g * GB, GB), GB), :] = mix.reshape(heads, GB, D)
        return carry

    lax.fori_loop(0, n_groups, group, 0)
    for g in range(n_groups):
        ko_copy(g).wait()
        vo_copy(g).wait()


def combine_kernel(dims, mix_ref, st_ref, wo_hbm, y_ref,
                   wo_vm, r_mix, r_st, c_t, o_s, p_send, p_recv, y_send, y_recv, y_all,
                   wo_sem, mix_ssem, mix_rsem, st_ssem, st_rsem, p_ssem, p_rsem, y_ssem, y_rsem,
                   a_ssem, a_rsem, f_ssem, f_rsem):
    groups, n_seq, n_head, n_groups, blk = dims
    head_i, seq_i = lax.axis_index("head"), lax.axis_index("seq")
    x_i, core_i = seq_i // 2, seq_i % 2
    n_x = n_seq // 2
    batch = n_groups * GB
    scale2 = (D ** -0.5) * LOG2E

    wo_copy = pltpu.make_async_copy(wo_hbm, wo_vm, wo_sem)
    wo_copy.start()
    barrier = pltpu.get_barrier_semaphore()
    for dh in range(n_head):
        for ds in range(n_seq):
            if dh or ds:
                pl.semaphore_signal(barrier, inc=1, device_id={
                    "head": (head_i + dh) % n_head, "seq": (seq_i + ds) % n_seq}, device_id_type=MESH)
    pl.semaphore_wait(barrier, n_head * n_seq - 1)

    copies = []
    for k in range(1, n_seq):
        to = (seq_i + k) % n_seq
        a = pltpu.make_async_remote_copy(st_ref, r_st.at[k - 1], st_ssem.at[k - 1], st_rsem.at[k - 1],
                                         device_id={"seq": to}, device_id_type=MESH)
        a.start()
        b = pltpu.make_async_remote_copy(mix_ref.at[pl.ds(to * groups, groups)], r_mix.at[k - 1],
                                         mix_ssem.at[k - 1], mix_rsem.at[k - 1],
                                         device_id={"seq": to}, device_id_type=MESH)
        b.start()
        copies.append((a, b))
    for a, b in copies:
        a.wait()
    ms = [st_ref[:n_groups]] + [r_st[k, :n_groups] for k in range(n_seq - 1)]
    ls = [st_ref[n_groups:]] + [r_st[k, n_groups:] for k in range(n_seq - 1)]
    top = functools.reduce(jnp.maximum, ms)
    es = [jnp.exp2((m - top) * scale2) for m in ms]
    total = functools.reduce(jnp.add, [l * e for l, e in zip(ls, es)])
    for k in range(n_seq):
        c_t[k] = (es[k] / total).T
    for a, b in copies:
        b.wait()
    for g in range(groups):
        tiles = []
        at = pl.ds(pl.multiple_of((seq_i * groups + g) * GB, GB), GB)
        cs = [c_t[k, at, :] for k in range(n_seq)]
        for n in range(n_groups):
            o = None
            for k in range(n_seq):
                src = mix_ref[seq_i * groups + g, n * GB:(n + 1) * GB, :] if k == 0 else r_mix[k - 1, g, n * GB:(n + 1) * GB, :]
                term = src * cs[k][:, n:n + 1]
                o = term if o is None else o + term
            tiles.append(o)
        o_s[:, g * D:(g + 1) * D] = jnp.concatenate(tiles, axis=0).astype(BF16)
    wo_copy.wait()

    def block_of(dh, dx, core):
        h, x = (head_i + dh) % n_head, (x_i + dx) % n_x
        return h, x * 2 + core, h * n_seq + x * 2 + core

    def product(b):
        return jnp.dot(o_s[...], wo_vm[:, pl.ds(pl.multiple_of(b * blk, blk), blk)], preferred_element_type=F32)

    order = [(dh, dx) for dh in range(n_head - 1, -1, -1) for dx in range(n_x - 1, -1, -1)]
    partner = {"seq": x_i * 2 + 1 - core_i}
    p_copies, y_copies = {}, {}
    for dh, dx in order:
        i = dh * n_x + dx
        _, _, b = block_of(dh, dx, 1 - core_i)
        p_send[i] = product(b)
        p_copies[i] = pltpu.make_async_remote_copy(p_send.at[i], p_recv.at[i], p_ssem.at[i], p_rsem.at[i],
                                                   device_id=partner, device_id_type=MESH)
        p_copies[i].start()
    own = None
    for dh, dx in order:
        i = dh * n_x + dx
        h, s, b = block_of(dh, dx, core_i)
        part = product(b)
        p_copies[i].wait_recv()
        part = part + p_recv[i]
        if i:
            y_send[i - 1] = part
            y_copies[i] = pltpu.make_async_remote_copy(y_send.at[i - 1], y_recv.at[i - 1], y_ssem.at[i - 1],
                                                       y_rsem.at[i - 1], device_id={"head": h, "seq": s},
                                                       device_id_type=MESH)
            y_copies[i].start()
        else:
            own = part
    for i in sorted(y_copies):
        y_copies[i].wait_recv()
        own = own + y_recv[i - 1]
    mine = head_i * n_seq + seq_i
    y_all[mine] = own.astype(BF16)
    gathers = {}
    for dh, dx in order:
        i = dh * n_x + dx
        h, s, b = block_of(dh, dx, core_i)
        if i:
            gathers[i] = pltpu.make_async_remote_copy(y_all.at[mine], y_all.at[mine], a_ssem.at[i - 1], a_rsem.at[i - 1],
                                                      device_id={"head": h, "seq": s}, device_id_type=MESH)
            gathers[i].start()
    forwards = {}
    for i in range(n_head * n_x):
        dh, dx = i // n_x, i % n_x
        _, _, b = block_of(dh, dx, core_i)
        if i:
            gathers[i].wait_recv()
        forwards[i] = pltpu.make_async_remote_copy(y_all.at[b], y_all.at[b], f_ssem.at[i], f_rsem.at[i],
                                                   device_id=partner, device_id_type=MESH)
        forwards[i].start()
    for i in forwards:
        forwards[i].wait()
    for i in p_copies:
        p_copies[i].wait_send()
    for i in y_copies:
        y_copies[i].wait_send()
        gathers[i].wait_send()
    for b in range(n_head * n_seq):
        y_ref[:, b * blk:(b + 1) * blk] = y_all[b]


def solution(mesh):
    n_head, n_seq = mesh.shape["head"], mesh.shape["seq"]
    cache_spec = P("rep", "seq", "head", None)

    def step(tokens, w_query, w_key, w_value, w_out, k_cache, v_cache, positions):
        batch, shard, kv, d = k_cache.shape
        model = tokens.shape[1]
        heads = w_query.shape[1] // d // n_head
        groups = heads // kv
        n_groups = batch // GB
        rows, lanes = shard * kv, heads * GB
        slots = 3
        any_spec = pl.BlockSpec(memory_space=pl.ANY)
        vmem = pl.BlockSpec(memory_space=pltpu.VMEM)
        flat = (batch, rows, d)
        dma = pltpu.SemaphoreType.DMA
        k_out, v_out, mix, stats = pl.pallas_call(
            functools.partial(attend_kernel, (kv, groups, shard, n_groups, slots)),
            name="attend",
            out_shape=(jax.ShapeDtypeStruct(flat, BF16), jax.ShapeDtypeStruct(flat, BF16),
                       jax.ShapeDtypeStruct((heads, batch, d), F32),
                       jax.ShapeDtypeStruct((2 * n_groups, lanes), F32)),
            in_specs=[pl.BlockSpec(memory_space=pltpu.SMEM), vmem] + [any_spec] * 5,
            out_specs=(any_spec, any_spec, vmem, vmem),
            scratch_shapes=[
                pltpu.VMEM(flat, BF16), pltpu.VMEM(flat, BF16),
                pltpu.VMEM((slots, model, kv * d), BF16),
                pltpu.VMEM((heads, batch, d), F32), pltpu.VMEM((kv, batch, d), F32),
                pltpu.VMEM((kv, batch, d), F32), pltpu.VMEM((rows // 8, 8, lanes), F32),
                dma((slots,)), dma((n_groups,)), dma((n_groups,)), dma((n_groups,)), dma((n_groups,)),
            ],
            compiler_params=pltpu.CompilerParams(vmem_limit_bytes=58 * MIB),
        )(positions, tokens, w_query, w_key, w_value, k_cache.reshape(flat), v_cache.reshape(flat))

        n_dev = n_head * n_seq
        blk = w_out.shape[1] // n_dev
        n_x = n_seq // 2
        chips = n_head * n_x
        y = pl.pallas_call(
            functools.partial(combine_kernel, (groups, n_seq, n_head, n_groups, blk)),
            name="combine",
            out_shape=jax.ShapeDtypeStruct((batch, w_out.shape[1]), BF16),
            in_specs=[vmem, vmem, any_spec],
            out_specs=vmem,
            scratch_shapes=[
                pltpu.VMEM(w_out.shape, BF16),
                pltpu.VMEM((n_seq - 1, groups, batch, d), F32), pltpu.VMEM((n_seq - 1, 2 * n_groups, lanes), F32),
                pltpu.VMEM((n_seq, lanes, n_groups), F32), pltpu.VMEM((batch, groups * d), BF16),
                pltpu.VMEM((chips, batch, blk), F32), pltpu.VMEM((chips, batch, blk), F32),
                pltpu.VMEM((chips - 1, batch, blk), F32), pltpu.VMEM((chips - 1, batch, blk), F32),
                pltpu.VMEM((n_dev, batch, blk), BF16),
                dma, dma((n_seq - 1,)), dma((n_seq - 1,)), dma((n_seq - 1,)), dma((n_seq - 1,)),
                dma((chips,)), dma((chips,)), dma((chips - 1,)), dma((chips - 1,)),
                dma((chips - 1,)), dma((chips - 1,)), dma((chips,)), dma((chips,)),
            ],
            compiler_params=pltpu.CompilerParams(collective_id=0, has_side_effects=True, vmem_limit_bytes=32 * MIB),
        )(mix, stats, w_out)
        return y, k_out.reshape(k_cache.shape), v_out.reshape(v_cache.shape)

    return jax.shard_map(
        step,
        mesh=mesh,
        in_specs=(P("rep", None), P(), P(), P(), P(("head", "seq"), None), cache_spec, cache_spec, P("rep")),
        out_specs=(P("rep", None), cache_spec, cache_spec),
        check_vma=False,
    )
```

```python
import functools

import jax
import jax.numpy as jnp
from jax import lax
from jax.experimental import pallas as pl
from jax.experimental.pallas import tpu as pltpu
from jax.sharding import PartitionSpec as P

MESH = pl.DeviceIdType.MESH
BF16 = jnp.bfloat16
F32 = jnp.float32
MIB = 2 ** 20
GB = 8
D = 128
LOG2E = 1.4426950408889634
SCALE2 = (D ** -0.5) * LOG2E
CHUNKS = ((0, 4), (4, 4))


def step_kernel(dims, pos_hbm, x_hbm, wq, wk, wv, wo_hbm, kc, vc, new_s, kv_vm, y_ref,
                pos_ref, x_vm, w_vm, wo_vm, q_s, s_s, wt_s, mix_s, st_s, r_mix, r_st, m_t, l_t, o_s,
                p_send, p_recv, y_send, y_recv, y_all,
                in_sem, w_sem, k_sem, v_sem, mix_ssem, mix_rsem, st_ssem, st_rsem,
                p_ssem, p_rsem, y_ssem, y_rsem, a_ssem, a_rsem, f_ssem, f_rsem):
    kv, groups, shard, n_groups, slots, n_seq, n_head, blk = dims
    heads = kv * groups
    rows = shard * kv
    lanes = heads * GB
    head_i, seq_i = lax.axis_index("head"), lax.axis_index("seq")
    x_i, core_i = seq_i // 2, seq_i % 2
    n_x = n_seq // 2
    base = seq_i * shard
    cols = kv * D
    n_q = heads // kv
    k_vm, v_vm, nk_s, nv_s = kv_vm.at[0], kv_vm.at[1], new_s.at[0], new_s.at[1]

    barrier = pltpu.get_barrier_semaphore()
    for dh in range(n_head):
        for ds in range(n_seq):
            if dh or ds:
                pl.semaphore_signal(barrier, inc=1, device_id={
                    "head": (head_i + dh) % n_head, "seq": (seq_i + ds) % n_seq}, device_id_type=MESH)

    def w_copy(c):
        if c < n_q:
            src, at = wq, head_i * (heads * D) + c * cols
        else:
            src, at = (wk, wv)[c - n_q], head_i * cols
        at = pl.multiple_of(at, cols)
        return pltpu.make_async_copy(src.at[:, pl.ds(at, cols)], w_vm.at[c % slots], w_sem.at[c % slots])

    def k_copy(g):
        at = pl.ds(g * GB, GB)
        return pltpu.make_async_copy(kc.at[at], k_vm.at[at], k_sem.at[g])

    def v_copy(g):
        at = pl.ds(g * GB, GB)
        return pltpu.make_async_copy(vc.at[at], v_vm.at[at], v_sem.at[g])

    x_copy = pltpu.make_async_copy(x_hbm, x_vm, in_sem.at[0])
    pos_copy = pltpu.make_async_copy(pos_hbm, pos_ref, in_sem.at[1])
    wo_copy = pltpu.make_async_copy(wo_hbm, wo_vm, in_sem.at[2])
    x_copy.start()
    pos_copy.start()

    n_w = n_q + 2
    ahead = 4
    for c in range(min(slots, n_w)):
        w_copy(c).start()
    issued = 0
    x_copy.wait()
    for c in range(n_w):
        w_copy(c).wait()
        r = jnp.dot(x_vm[...], w_vm[c % slots], preferred_element_type=F32)
        r = r.astype(BF16).astype(F32)
        for i in range(kv):
            part = r[:, i * D:(i + 1) * D]
            if c < n_q:
                q_s[c * kv + i] = part
            elif c == n_q:
                nk_s[i] = part
            else:
                nv_s[i] = part
        if c + slots < n_w:
            w_copy(c + slots).start()
        else:
            while issued < min(ahead, n_groups) and issued <= (c + slots - n_w + 1):
                k_copy(issued).start()
                v_copy(issued).start()
                issued += 1
    for g in range(issued, min(ahead, n_groups)):
        k_copy(g).start()
        v_copy(g).start()
    pos_copy.wait()

    sub = lax.broadcasted_iota(jnp.int32, (8, lanes), 0)
    lane = lax.broadcasted_iota(jnp.int32, (8, lanes), 1)
    lane_d = lax.broadcasted_iota(jnp.int32, (D, lanes), 1)
    row_l = lax.broadcasted_iota(jnp.int32, (lanes, D), 0)
    per_tile = 8 // kv
    half = rows // 2

    def rows_of(g):
        return pl.ds(pl.multiple_of(g * GB, GB), GB)

    def scores(g):
        q_t = q_s[:, rows_of(g), :].reshape(lanes, D).T
        accs = [None, None]
        for p in range(GB // 2):
            qs = jnp.concatenate([jnp.where(lane_d % GB == 2 * p, q_t, 0.0),
                                  jnp.where(lane_d % GB == 2 * p + 1, q_t, 0.0)], axis=0).astype(BF16)
            for h in range(2):
                at = pl.ds(h * half, half)
                keys = jnp.concatenate([k_vm[g * GB + 2 * p, at, :], k_vm[g * GB + 2 * p + 1, at, :]], axis=1)
                s = jnp.dot(keys, qs, preferred_element_type=F32)
                accs[h] = s if accs[h] is None else accs[h] + s
        for h in range(2):
            s_s[pl.ds(h * (half // 8), half // 8)] = accs[h].reshape(half // 8, 8, lanes)

    def softmax(g):
        pos_row = jnp.zeros((8, lanes), jnp.int32)
        for i in range(GB):
            pos_row = jnp.where(lane % GB == i, pos_ref[g * GB + i] - base, pos_row)
        limit = jnp.where(sub % kv == lane // (groups * GB), pos_row - 1 - sub // kv, -1)
        tile_t = lax.broadcasted_iota(jnp.int32, (rows // 8, 8, lanes), 0) * per_tile
        s3 = jnp.where(limit[None] >= tile_t, s_s[...], -jnp.inf)
        m = jnp.max(jnp.max(s3, axis=0), axis=0, keepdims=True)
        m_safe = jnp.where(m > -jnp.inf, m, 0.0)
        w3 = jnp.exp2((s3 - m_safe[None]) * SCALE2)
        total = jnp.sum(jnp.sum(w3, axis=0), axis=0, keepdims=True)
        st_s[g] = jnp.where(sub == 0, m, total)
        wt_s[...] = w3.reshape(rows, lanes).astype(BF16).T

    def values(g):
        mix = jnp.zeros((lanes, D), F32)
        for p in range(GB // 2):
            vals = jnp.concatenate([v_vm[g * GB + 2 * p], v_vm[g * GB + 2 * p + 1]], axis=1)
            o = jnp.dot(wt_s[...], vals, preferred_element_type=F32)
            mix = jnp.where(row_l % GB == 2 * p, o[:, :D], mix)
            mix = jnp.where(row_l % GB == 2 * p + 1, o[:, D:], mix)
        mix_s[:, rows_of(g), :] = mix.reshape(heads, GB, D)

    def mix_copy(g, k):
        to = (seq_i + k) % n_seq
        return pltpu.make_async_remote_copy(
            mix_s.at[pl.ds(to * groups, groups), rows_of(g)], r_mix.at[k - 1, :, rows_of(g)],
            mix_ssem.at[g, k - 1], mix_rsem.at[g, k - 1], device_id={"seq": to}, device_id_type=MESH)

    def st_copy(g, k):
        to = (seq_i + k) % n_seq
        return pltpu.make_async_remote_copy(st_s.at[g], r_st.at[k - 1, g], st_ssem.at[g, k - 1], st_rsem.at[g, k - 1],
                                            device_id={"seq": to}, device_id_type=MESH)

    order = [(dh, dx) for dh in range(n_head - 1, -1, -1) for dx in range(n_x - 1, -1, -1)]
    partner = {"seq": x_i * 2 + 1 - core_i}
    mine = head_i * n_seq + seq_i

    def block_of(dh, dx, core):
        h, x = (head_i + dh) % n_head, (x_i + dx) % n_x
        return h, x * 2 + core, h * n_seq + x * 2 + core

    def p_copy(c, i):
        at = pl.ds(CHUNKS[c][0] * GB, CHUNKS[c][1] * GB)
        return pltpu.make_async_remote_copy(p_send.at[i, at], p_recv.at[i, at], p_ssem.at[c, i], p_rsem.at[c, i],
                                            device_id=partner, device_id_type=MESH)

    def y_copy(c, dh, dx):
        i = dh * n_x + dx
        at = pl.ds(CHUNKS[c][0] * GB, CHUNKS[c][1] * GB)
        h, s, _ = block_of(dh, dx, core_i)
        return pltpu.make_async_remote_copy(y_send.at[i, at], y_recv.at[i - 1, at], y_ssem.at[c, i - 1],
                                            y_rsem.at[c, i - 1], device_id={"head": h, "seq": s}, device_id_type=MESH)

    def a_copy(c, dh, dx):
        i = dh * n_x + dx
        at = pl.ds(CHUNKS[c][0] * GB, CHUNKS[c][1] * GB)
        h, s, _ = block_of(dh, dx, core_i)
        return pltpu.make_async_remote_copy(y_all.at[mine, at], y_all.at[mine, at], a_ssem.at[c, i - 1],
                                            a_rsem.at[c, i - 1], device_id={"head": h, "seq": s}, device_id_type=MESH)

    def f_copy(c, dh, dx):
        i = dh * n_x + dx
        at = pl.ds(CHUNKS[c][0] * GB, CHUNKS[c][1] * GB)
        _, _, b = block_of(dh, dx, core_i)
        return pltpu.make_async_remote_copy(y_all.at[b, at], y_all.at[b, at], f_ssem.at[c, i], f_rsem.at[c, i],
                                            device_id=partner, device_id_type=MESH)

    def out_products(c):
        g0, n = CHUNKS[c]
        for g in range(g0, g0 + n):
            for k in range(1, n_seq):
                st_copy(g, k).wait()
        own_rows = pl.ds(pl.multiple_of(seq_i * groups * GB, groups * GB), groups * GB)
        for k in range(n_seq):
            src = st_s if k == 0 else r_st.at[k - 1]
            m_t[k] = jnp.concatenate([src[g, 0:1, :] for g in range(g0, g0 + n)], axis=0).T
            l_t[k] = jnp.concatenate([src[g, 1:2, :] for g in range(g0, g0 + n)], axis=0).T
        ms = [m_t[k, own_rows, :] for k in range(n_seq)]
        ls = [l_t[k, own_rows, :] for k in range(n_seq)]
        col = lax.broadcasted_iota(jnp.int32, (GB, n), 1)
        fresh = []
        for j in range(groups):
            s_new = jnp.zeros((GB, n), F32)
            for t in range(n):
                at = pl.ds((g0 + t) * GB, GB)
                dot = jnp.sum(q_s[seq_i * groups + j, at, :] * nk_s[seq_i, at, :], axis=1, keepdims=True)
                s_new = jnp.where(col == t, dot, s_new)
            fresh.append(s_new)
        m_new = jnp.concatenate(fresh, axis=0)
        top = functools.reduce(jnp.maximum, ms + [m_new])
        es = [jnp.exp2((m - top) * SCALE2) for m in ms]
        e_new = jnp.exp2((m_new - top) * SCALE2)
        total = functools.reduce(jnp.add, [l * e for l, e in zip(ls, es)] + [e_new])
        cs = [e / total for e in es]
        c_new = e_new / total
        for g in range(g0, g0 + n):
            for k in range(1, n_seq):
                mix_copy(g, k).wait()
        for j in range(groups):
            tiles = []
            for t in range(n):
                at = pl.ds((g0 + t) * GB, GB)
                o = nv_s[seq_i, at, :] * c_new[j * GB:(j + 1) * GB, t:t + 1]
                for k in range(n_seq):
                    src = mix_s[seq_i * groups + j, at, :] if k == 0 else r_mix[k - 1, j, at, :]
                    o = o + src * cs[k][j * GB:(j + 1) * GB, t:t + 1]
                tiles.append(o)
            o_s[pl.ds(g0 * GB, n * GB), j * D:(j + 1) * D] = jnp.concatenate(tiles, axis=0).astype(BF16)
        at = pl.ds(g0 * GB, n * GB)
        o = o_s[at, :]

        def product(b):
            return jnp.dot(o, wo_vm[:, pl.ds(pl.multiple_of(b * blk, blk), blk)], preferred_element_type=F32)

        for dh, dx in order:
            i = dh * n_x + dx
            p_send[i, at, :] = product(block_of(dh, dx, 1 - core_i)[2])
            p_copy(c, i).start()
        for dh, dx in order:
            y_send[dh * n_x + dx, at, :] = product(block_of(dh, dx, core_i)[2])

    def out_scatter(c):
        at = pl.ds(CHUNKS[c][0] * GB, CHUNKS[c][1] * GB)
        for dh, dx in order:
            i = dh * n_x + dx
            p_copy(c, i).wait_recv()
            y_send[i, at, :] = y_send[i, at, :] + p_recv[i, at, :]
            if i:
                y_copy(c, dh, dx).start()

    def out_gather(c):
        at = pl.ds(CHUNKS[c][0] * GB, CHUNKS[c][1] * GB)
        own = y_send[0, at, :]
        for dh, dx in reversed(order[:-1]):
            y_copy(c, dh, dx).wait_recv()
            own = own + y_recv[dh * n_x + dx - 1, at, :]
        y_all[mine, at, :] = own.astype(BF16)
        for dh, dx in order[:-1]:
            a_copy(c, dh, dx).start()
        f_copy(c, 0, 0).start()

    def out_forward(c):
        for dh, dx in reversed(order[:-1]):
            a_copy(c, dh, dx).wait_recv()
            f_copy(c, dh, dx).start()

    def out_finish(c):
        for dh, dx in order:
            f_copy(c, dh, dx).wait()
            p_copy(c, dh * n_x + dx).wait_send()
            if dh or dx:
                y_copy(c, dh, dx).wait_send()
                a_copy(c, dh, dx).wait_send()

    k_copy(0).wait()
    scores(0)
    softmax(0)
    pl.semaphore_wait(barrier, n_head * n_seq - 1)
    wo_copy.start()

    def group(g, carry):
        @pl.when(g + ahead < n_groups)
        def _():
            k_copy(g + ahead).start()
            v_copy(g + ahead).start()
        v_copy(g).wait()
        k_copy(g + 1).wait()
        scores(g + 1)
        values(g)
        for k in range(1, n_seq):
            st_copy(g, k).start()
            mix_copy(g, k).start()
        softmax(g + 1)

        @pl.when(g == 4)
        def _():
            wo_copy.wait()
            out_products(0)

        @pl.when(g == 5)
        def _():
            out_scatter(0)

        return carry

    lax.fori_loop(0, n_groups - 1, group, 0)
    last = n_groups - 1
    v_copy(last).wait()
    values(last)
    for k in range(1, n_seq):
        st_copy(last, k).start()
        mix_copy(last, k).start()
    out_gather(0)
    out_products(1)
    out_scatter(1)
    out_forward(0)
    out_gather(1)
    out_forward(1)
    out_finish(0)
    out_finish(1)
    for b in range(n_head * n_seq):
        y_ref[:, b * blk:(b + 1) * blk] = y_all[b]


def write_kernel(dims, pos_ref, new, kv_new, ko, vo, patch, o_sem, p_sem):
    shard, n_groups = dims
    batch = n_groups * GB
    base = lax.axis_index("seq") * shard
    outs = (ko, vo)

    def copy(side, g):
        at = pl.ds(g * GB, GB)
        return pltpu.make_async_copy(kv_new.at[side, at], outs[side].at[at], o_sem.at[side, g])

    def patch_copy(side, b, t):
        return pltpu.make_async_copy(patch.at[side, b], outs[side].at[b, t], p_sem.at[side, b])

    def place(b):
        t = pos_ref[b] - base
        return t, jnp.logical_and(t >= 0, t < shard)

    for side in range(2):
        for g in range(n_groups):
            copy(side, g).start()

    def patch_rows(b, carry):
        for side in range(2):
            patch[side, b] = new[side, :, b, :].astype(BF16)
        return carry

    lax.fori_loop(0, batch, patch_rows, 0)
    for side in range(2):
        for g in range(n_groups):
            copy(side, g).wait()
            for i in range(GB):
                b = g * GB + i
                t, hit = place(b)

                @pl.when(hit)
                def _():
                    patch_copy(side, b, t).start()

    def finish(b, carry):
        t, hit = place(b)

        @pl.when(hit)
        def _():
            patch_copy(0, b, t).wait()
            patch_copy(1, b, t).wait()
        return carry

    lax.fori_loop(0, batch, finish, 0)


def solution(mesh):
    n_head, n_seq = mesh.shape["head"], mesh.shape["seq"]
    cache_spec = P("rep", "seq", "head", None)

    def step(tokens, w_query, w_key, w_value, w_out, k_cache, v_cache, positions):
        batch, shard, kv, d = k_cache.shape
        model = tokens.shape[1]
        heads = w_query.shape[1] // d // n_head
        groups = heads // kv
        n_groups = batch // GB
        rows, lanes = shard * kv, heads * GB
        slots = 3
        n_dev = n_head * n_seq
        blk = w_out.shape[1] // n_dev
        chips = n_head * (n_seq // 2)
        n_c = len(CHUNKS)
        c_groups = CHUNKS[0][1]
        hbm = pl.BlockSpec(memory_space=pltpu.HBM)
        any_spec = pl.BlockSpec(memory_space=pl.ANY)
        vmem = pl.BlockSpec(memory_space=pltpu.VMEM)
        flat = (batch, rows, d)
        dma = pltpu.SemaphoreType.DMA
        fresh, kv_raw, y = pl.pallas_call(
            functools.partial(step_kernel, (kv, groups, shard, n_groups, slots, n_seq, n_head, blk)),
            name="step",
            out_shape=(pltpu.VMEM((2, kv, batch, d), F32), pltpu.VMEM((2, *flat), BF16),
                       jax.ShapeDtypeStruct((batch, w_out.shape[1]), BF16)),
            in_specs=[hbm] * 8,
            out_specs=(vmem,) * 3,
            scratch_shapes=[
                pltpu.SMEM((batch,), jnp.int32), pltpu.VMEM((batch, model), BF16),
                pltpu.VMEM((slots, model, kv * d), BF16), pltpu.VMEM(w_out.shape, BF16),
                pltpu.VMEM((heads, batch, d), F32), pltpu.VMEM((rows // 8, 8, lanes), F32),
                pltpu.VMEM((lanes, rows), BF16), pltpu.VMEM((heads, batch, d), F32),
                pltpu.VMEM((n_groups, 8, lanes), F32),
                pltpu.VMEM((n_seq - 1, groups, batch, d), F32), pltpu.VMEM((n_seq - 1, n_groups, 8, lanes), F32),
                pltpu.VMEM((n_seq, lanes, c_groups), F32), pltpu.VMEM((n_seq, lanes, c_groups), F32),
                pltpu.VMEM((batch, groups * d), BF16),
                pltpu.VMEM((chips, batch, blk), F32), pltpu.VMEM((chips, batch, blk), F32),
                pltpu.VMEM((chips, batch, blk), F32), pltpu.VMEM((chips - 1, batch, blk), F32),
                pltpu.VMEM((n_dev, batch, blk), BF16),
                dma((3,)), dma((slots,)), dma((n_groups,)), dma((n_groups,)),
                dma((n_groups, n_seq - 1)), dma((n_groups, n_seq - 1)),
                dma((n_groups, n_seq - 1)), dma((n_groups, n_seq - 1)),
                dma((n_c, chips)), dma((n_c, chips)), dma((n_c, chips - 1)), dma((n_c, chips - 1)),
                dma((n_c, chips - 1)), dma((n_c, chips - 1)), dma((n_c, chips)), dma((n_c, chips)),
            ],
            compiler_params=pltpu.CompilerParams(collective_id=0, has_side_effects=True, vmem_limit_bytes=28 * MIB),
        )(positions, tokens, w_query, w_key, w_value, w_out, k_cache.reshape(flat), v_cache.reshape(flat))

        k_out, v_out = pl.pallas_call(
            functools.partial(write_kernel, (shard, n_groups)), name="write",
            out_shape=(jax.ShapeDtypeStruct(k_cache.shape, BF16), jax.ShapeDtypeStruct(k_cache.shape, BF16)),
            in_specs=[pl.BlockSpec(memory_space=pltpu.SMEM), vmem, any_spec],
            out_specs=(any_spec, any_spec),
            scratch_shapes=[pltpu.VMEM((2, batch, kv, d), BF16), dma((2, n_groups)), dma((2, batch))],
            compiler_params=pltpu.CompilerParams(vmem_limit_bytes=4 * MIB),
        )(positions, fresh, kv_raw.reshape(2, *k_cache.shape))
        return y, k_out, v_out

    return jax.shard_map(
        step,
        mesh=mesh,
        in_specs=(P("rep", None), P(), P(), P(), P(("head", "seq"), None), cache_spec, cache_spec, P("rep")),
        out_specs=(P("rep", None), cache_spec, cache_spec),
        check_vma=False,
    )
```

```python
import functools

import jax
import jax.numpy as jnp
from jax import lax
from jax.experimental import pallas as pl
from jax.experimental.pallas import tpu as pltpu
from jax.sharding import PartitionSpec as P

MESH = pl.DeviceIdType.MESH
BF16 = jnp.bfloat16
F32 = jnp.float32
MIB = 2 ** 20
GB = 8
D = 128
LOG2E = 1.4426950408889634
SCALE2 = (D ** -0.5) * LOG2E
CHUNKS = ((0, 4), (4, 4))


def step_kernel(dims, pos_hbm, x_hbm, wq, wk, wv, wo_hbm, kc, vc, new_s, y_ref, kv_vm,
                pos_ref, x_vm, w_vm, wo_vm, q_s, s_s, wt_s, mix_s, st_s, r_mix, r_st, m_t, l_t, o_s,
                p_send, p_recv, y_send, y_recv, y_all,
                in_sem, w_sem, k_sem, v_sem, h_ssem, h_rsem, mix_ssem, mix_rsem, st_ssem, st_rsem,
                p_ssem, p_rsem, y_ssem, y_rsem, a_ssem, a_rsem, f_ssem, f_rsem):
    kv, groups, shard, n_groups, slots, n_seq, n_head, blk = dims
    heads = kv * groups
    rows = shard * kv
    lanes = heads * GB
    head_i, seq_i = lax.axis_index("head"), lax.axis_index("seq")
    x_i, core_i = seq_i // 2, seq_i % 2
    n_x = n_seq // 2
    base = seq_i * shard
    cols = kv * D
    n_q = heads // kv
    partner = {"seq": x_i * 2 + 1 - core_i}
    k_vm, v_vm, nk_s, nv_s = kv_vm.at[0], kv_vm.at[1], new_s.at[0], new_s.at[1]

    barrier = pltpu.get_barrier_semaphore()
    for dh in range(n_head):
        for ds in range(n_seq):
            if dh or ds:
                pl.semaphore_signal(barrier, inc=1, device_id={
                    "head": (head_i + dh) % n_head, "seq": (seq_i + ds) % n_seq}, device_id_type=MESH)

    half_cols = cols // 2
    q_mine = n_q // 2

    def w_copies(c):
        if c < q_mine:
            at = pl.multiple_of(head_i * (heads * D) + (core_i * q_mine + c) * cols, cols)
            return [pltpu.make_async_copy(wq.at[:, pl.ds(at, cols)], w_vm.at[c], w_sem.at[c])]
        at = pl.multiple_of(head_i * cols + core_i * half_cols, half_cols)
        return [pltpu.make_async_copy(src.at[:, pl.ds(at, half_cols)], w_vm.at[c, :, pl.ds(n * half_cols, half_cols)],
                                      w_sem.at[c + n]) for n, src in enumerate((wk, wv))]

    def k_copy(g):
        at = pl.ds(g * GB, GB)
        return pltpu.make_async_copy(kc.at[at], k_vm.at[at], k_sem.at[g])

    def v_copy(g):
        at = pl.ds(g * GB, GB)
        return pltpu.make_async_copy(vc.at[at], v_vm.at[at], v_sem.at[g])

    x_copy = pltpu.make_async_copy(x_hbm, x_vm, in_sem.at[0])
    pos_copy = pltpu.make_async_copy(pos_hbm, pos_ref, in_sem.at[1])
    wo_copy = pltpu.make_async_copy(wo_hbm, wo_vm, in_sem.at[2])
    x_copy.start()
    pos_copy.start()

    ahead = 4
    for c in range(q_mine + 1):
        for copy in w_copies(c):
            copy.start()
    x_copy.wait()
    hq = heads // 2
    q_part = q_s.at[:, pl.ds(pl.multiple_of(core_i * hq, hq), hq)]
    n_part = new_s.at[:, pl.ds(core_i * (kv // 2), kv // 2)]
    q_share = pltpu.make_async_remote_copy(q_part, q_part, h_ssem.at[0], h_rsem.at[0],
                                           device_id=partner, device_id_type=MESH)
    n_share = pltpu.make_async_remote_copy(n_part, n_part, h_ssem.at[1], h_rsem.at[1],
                                           device_id=partner, device_id_type=MESH)
    for c in range(q_mine + 1):
        for copy in w_copies(c):
            copy.wait()
        if c < ahead:
            k_copy(c).start()
            v_copy(c).start()
        r = jnp.dot(x_vm[...], w_vm[c], preferred_element_type=F32)
        r = r.astype(BF16).astype(F32)
        if c < q_mine:
            for i in range(kv):
                q_s[:, core_i * hq + c * kv + i, :] = r[:, i * D:(i + 1) * D]
        else:
            for n in range(2):
                for i in range(kv // 2):
                    new_s[n, core_i * (kv // 2) + i] = r[:, n * half_cols + i * D:n * half_cols + (i + 1) * D]
        if c == q_mine - 1:
            pl.semaphore_wait(barrier, n_head * n_seq - 1)
            q_share.start()
    n_share.start()
    for g in range(q_mine + 1, ahead):
        k_copy(g).start()
        v_copy(g).start()
    q_share.wait()
    n_share.wait()
    pos_copy.wait()

    sub = lax.broadcasted_iota(jnp.int32, (8, lanes), 0)
    lane = lax.broadcasted_iota(jnp.int32, (8, lanes), 1)
    lane_d = lax.broadcasted_iota(jnp.int32, (D, lanes), 1)
    per_tile = 8 // kv
    half = rows // 2

    def rows_of(g):
        return pl.ds(pl.multiple_of(g * GB, GB), GB)

    def scores(g):
        q_t = q_s[rows_of(g)].reshape(lanes, D).T
        accs = [None, None]
        for p in range(GB // 2):
            qs = jnp.concatenate([jnp.where(lane_d // heads == 2 * p, q_t, 0.0),
                                  jnp.where(lane_d // heads == 2 * p + 1, q_t, 0.0)], axis=0).astype(BF16)
            for h in range(2):
                at = pl.ds(h * half, half)
                keys = jnp.concatenate([k_vm[g * GB + 2 * p, at, :], k_vm[g * GB + 2 * p + 1, at, :]], axis=1)
                s = jnp.dot(keys, qs, preferred_element_type=F32)
                accs[h] = s if accs[h] is None else accs[h] + s
        for h in range(2):
            s_s[pl.ds(h * (half // 8), half // 8)] = accs[h].reshape(half // 8, 8, lanes)

    def softmax(g):
        pos_row = jnp.zeros((8, lanes), jnp.int32)
        for i in range(GB):
            pos_row = jnp.where(lane // heads == i, pos_ref[g * GB + i] - base, pos_row)
        limit = jnp.where(sub % kv == lane % heads // groups, pos_row - 1 - sub // kv, -1)
        tile_t = lax.broadcasted_iota(jnp.int32, (rows // 8, 8, lanes), 0) * per_tile
        s3 = jnp.where(limit[None] >= tile_t, s_s[...], -jnp.inf)
        m = jnp.max(jnp.max(s3, axis=0), axis=0, keepdims=True)
        m_safe = jnp.where(m > -jnp.inf, m, 0.0)
        w3 = jnp.exp2((s3 - m_safe[None]) * SCALE2)
        total = jnp.sum(jnp.sum(w3, axis=0), axis=0, keepdims=True)
        st_s[g] = jnp.where(sub == 0, m, total)
        wt_s[...] = w3.reshape(rows, lanes).astype(BF16).T

    def values(g):
        for i in range(GB):
            b = g * GB + i
            mix_s[:, b, :] = jnp.dot(wt_s[i * heads:(i + 1) * heads, :], v_vm[b], preferred_element_type=F32)

    def mix_copy(g, k):
        to = (seq_i + k) % n_seq
        return pltpu.make_async_remote_copy(
            mix_s.at[pl.ds(to * groups, groups), rows_of(g)], r_mix.at[k - 1, :, rows_of(g)],
            mix_ssem.at[g, k - 1], mix_rsem.at[g, k - 1], device_id={"seq": to}, device_id_type=MESH)

    def st_copy(g, k):
        to = (seq_i + k) % n_seq
        return pltpu.make_async_remote_copy(st_s.at[g], r_st.at[k - 1, g], st_ssem.at[g, k - 1], st_rsem.at[g, k - 1],
                                            device_id={"seq": to}, device_id_type=MESH)

    order = [(dh, dx) for dh in range(n_head - 1, -1, -1) for dx in range(n_x - 1, -1, -1)]
    mine = head_i * n_seq + seq_i

    def block_of(dh, dx, core):
        h, x = (head_i + dh) % n_head, (x_i + dx) % n_x
        return h, x * 2 + core, h * n_seq + x * 2 + core

    def p_copy(c, i):
        at = pl.ds(CHUNKS[c][0] * GB, CHUNKS[c][1] * GB)
        return pltpu.make_async_remote_copy(p_send.at[i, at], p_recv.at[i, at], p_ssem.at[c, i], p_rsem.at[c, i],
                                            device_id=partner, device_id_type=MESH)

    def y_copy(c, dh, dx):
        i = dh * n_x + dx
        at = pl.ds(CHUNKS[c][0] * GB, CHUNKS[c][1] * GB)
        h, s, _ = block_of(dh, dx, core_i)
        return pltpu.make_async_remote_copy(y_send.at[i, at], y_recv.at[i - 1, at], y_ssem.at[c, i - 1],
                                            y_rsem.at[c, i - 1], device_id={"head": h, "seq": s}, device_id_type=MESH)

    def a_copy(c, dh, dx):
        i = dh * n_x + dx
        at = pl.ds(CHUNKS[c][0] * GB, CHUNKS[c][1] * GB)
        h, s, _ = block_of(dh, dx, core_i)
        return pltpu.make_async_remote_copy(y_all.at[mine, at], y_all.at[mine, at], a_ssem.at[c, i - 1],
                                            a_rsem.at[c, i - 1], device_id={"head": h, "seq": s}, device_id_type=MESH)

    def f_copy(c, dh, dx):
        i = dh * n_x + dx
        at = pl.ds(CHUNKS[c][0] * GB, CHUNKS[c][1] * GB)
        _, _, b = block_of(dh, dx, core_i)
        return pltpu.make_async_remote_copy(y_all.at[b, at], y_all.at[b, at], f_ssem.at[c, i], f_rsem.at[c, i],
                                            device_id=partner, device_id_type=MESH)

    def out_products(c):
        g0, n = CHUNKS[c]
        for g in range(g0, g0 + n):
            for k in range(1, n_seq):
                st_copy(g, k).wait()
        for k in range(n_seq):
            src = st_s if k == 0 else r_st.at[k - 1]
            m_t[k] = jnp.concatenate([src[g, 0:1, :] for g in range(g0, g0 + n)], axis=0).T
            l_t[k] = jnp.concatenate([src[g, 1:2, :] for g in range(g0, g0 + n)], axis=0).T

        def own(ref, k):
            return jnp.concatenate([ref[k, pl.ds(seq_i * groups + j, GB, stride=heads), :] for j in range(groups)], axis=0)

        ms = [own(m_t, k) for k in range(n_seq)]
        ls = [own(l_t, k) for k in range(n_seq)]
        col = lax.broadcasted_iota(jnp.int32, (GB, n), 1)
        fresh = []
        for j in range(groups):
            s_new = jnp.zeros((GB, n), F32)
            for t in range(n):
                at = pl.ds((g0 + t) * GB, GB)
                dot = jnp.sum(q_s[at, seq_i * groups + j, :] * nk_s[seq_i, at, :], axis=1, keepdims=True)
                s_new = jnp.where(col == t, dot, s_new)
            fresh.append(s_new)
        m_new = jnp.concatenate(fresh, axis=0)
        top = functools.reduce(jnp.maximum, ms + [m_new])
        es = [jnp.exp2((m - top) * SCALE2) for m in ms]
        e_new = jnp.exp2((m_new - top) * SCALE2)
        total = functools.reduce(jnp.add, [l * e for l, e in zip(ls, es)] + [e_new])
        cs = [e / total for e in es]
        c_new = e_new / total
        for g in range(g0, g0 + n):
            for k in range(1, n_seq):
                mix_copy(g, k).wait()
        for j in range(groups):
            tiles = []
            for t in range(n):
                at = pl.ds((g0 + t) * GB, GB)
                o = nv_s[seq_i, at, :] * c_new[j * GB:(j + 1) * GB, t:t + 1]
                for k in range(n_seq):
                    src = mix_s[seq_i * groups + j, at, :] if k == 0 else r_mix[k - 1, j, at, :]
                    o = o + src * cs[k][j * GB:(j + 1) * GB, t:t + 1]
                tiles.append(o)
            o_s[pl.ds(g0 * GB, n * GB), j * D:(j + 1) * D] = jnp.concatenate(tiles, axis=0).astype(BF16)
        at = pl.ds(g0 * GB, n * GB)
        o = o_s[at, :]

        def product(b):
            return jnp.dot(o, wo_vm[:, pl.ds(pl.multiple_of(b * blk, blk), blk)], preferred_element_type=F32)

        for dh, dx in order:
            i = dh * n_x + dx
            p_send[i, at, :] = product(block_of(dh, dx, 1 - core_i)[2])
            p_copy(c, i).start()
        for dh, dx in order:
            y_send[dh * n_x + dx, at, :] = product(block_of(dh, dx, core_i)[2])

    def out_scatter(c):
        at = pl.ds(CHUNKS[c][0] * GB, CHUNKS[c][1] * GB)
        for dh, dx in order:
            i = dh * n_x + dx
            p_copy(c, i).wait_recv()
            y_send[i, at, :] = y_send[i, at, :] + p_recv[i, at, :]
            if i:
                y_copy(c, dh, dx).start()

    def out_gather(c):
        at = pl.ds(CHUNKS[c][0] * GB, CHUNKS[c][1] * GB)
        own = y_send[0, at, :]
        for dh, dx in reversed(order[:-1]):
            y_copy(c, dh, dx).wait_recv()
            own = own + y_recv[dh * n_x + dx - 1, at, :]
        y_all[mine, at, :] = own.astype(BF16)
        for dh, dx in order[:-1]:
            a_copy(c, dh, dx).start()
        f_copy(c, 0, 0).start()

    def out_forward(c):
        for dh, dx in reversed(order[:-1]):
            a_copy(c, dh, dx).wait_recv()
            f_copy(c, dh, dx).start()

    def out_finish(c):
        for dh, dx in order:
            f_copy(c, dh, dx).wait()
            p_copy(c, dh * n_x + dx).wait_send()
            if dh or dx:
                y_copy(c, dh, dx).wait_send()
                a_copy(c, dh, dx).wait_send()

    k_copy(0).wait()
    scores(0)
    softmax(0)
    wo_copy.start()

    def group(g, carry):
        @pl.when(g + ahead < n_groups)
        def _():
            k_copy(g + ahead).start()
            v_copy(g + ahead).start()
        v_copy(g).wait()
        k_copy(g + 1).wait()
        scores(g + 1)
        values(g)
        for k in range(1, n_seq):
            st_copy(g, k).start()
            mix_copy(g, k).start()
        softmax(g + 1)

        @pl.when(g == 4)
        def _():
            wo_copy.wait()
            out_products(0)

        @pl.when(g == 5)
        def _():
            out_scatter(0)

        return carry

    lax.fori_loop(0, n_groups - 1, group, 0)
    last = n_groups - 1
    v_copy(last).wait()
    values(last)
    for k in range(1, n_seq):
        st_copy(last, k).start()
        mix_copy(last, k).start()
    out_gather(0)
    out_products(1)
    out_scatter(1)
    out_forward(0)
    out_gather(1)
    out_forward(1)
    out_finish(0)
    out_finish(1)
    for b in range(n_head * n_seq):
        y_ref[:, b * blk:(b + 1) * blk] = y_all[b]


def write_kernel(dims, pos_ref, new, y_in, kv_in, ko, vo, y_out, kv_vm, o_sem, y_sem):
    shard, n_groups = dims
    del kv_in
    base = lax.axis_index("seq") * shard
    outs = (ko, vo)
    copies = [pltpu.make_async_copy(y_in, y_out, y_sem)]
    copies[0].start()
    for g in range(n_groups):
        for i in range(GB):
            b = g * GB + i
            t = pos_ref[b] - base

            @pl.when(jnp.logical_and(t >= 0, t < shard))
            def _():
                for side in range(2):
                    kv_vm[side, b, t] = new[side, :, b, :].astype(BF16)

        at = pl.ds(g * GB, GB)
        for side in range(2):
            copies.append(pltpu.make_async_copy(kv_vm.at[side, at], outs[side].at[at], o_sem.at[side, g]))
            copies[-1].start()
    for c in copies:
        c.wait()


def solution(mesh):
    n_head, n_seq = mesh.shape["head"], mesh.shape["seq"]
    cache_spec = P("rep", "seq", "head", None)

    def step(tokens, w_query, w_key, w_value, w_out, k_cache, v_cache, positions):
        batch, shard, kv, d = k_cache.shape
        model = tokens.shape[1]
        heads = w_query.shape[1] // d // n_head
        groups = heads // kv
        n_groups = batch // GB
        rows, lanes = shard * kv, heads * GB
        slots = heads // kv // 2 + 1
        n_dev = n_head * n_seq
        blk = w_out.shape[1] // n_dev
        chips = n_head * (n_seq // 2)
        n_c = len(CHUNKS)
        c_groups = CHUNKS[0][1]
        hbm = pl.BlockSpec(memory_space=pltpu.HBM)
        any_spec = pl.BlockSpec(memory_space=pl.ANY)
        vmem = pl.BlockSpec(memory_space=pltpu.VMEM)
        flat = (batch, rows, d)
        dma = pltpu.SemaphoreType.DMA
        fresh, y, kv_raw = pl.pallas_call(
            functools.partial(step_kernel, (kv, groups, shard, n_groups, slots, n_seq, n_head, blk)),
            name="step",
            out_shape=(pltpu.VMEM((2, kv, batch, d), F32), pltpu.VMEM((batch, w_out.shape[1]), BF16),
                       pltpu.VMEM((2, *flat), BF16)),
            in_specs=[hbm] * 8,
            out_specs=(vmem,) * 3,
            scratch_shapes=[
                pltpu.SMEM((batch,), jnp.int32), pltpu.VMEM((batch, model), BF16),
                pltpu.VMEM((slots, model, kv * d), BF16), pltpu.VMEM(w_out.shape, BF16),
                pltpu.VMEM((batch, heads, d), F32), pltpu.VMEM((rows // 8, 8, lanes), F32),
                pltpu.VMEM((lanes, rows), BF16), pltpu.VMEM((heads, batch, d), F32),
                pltpu.VMEM((n_groups, 8, lanes), F32),
                pltpu.VMEM((n_seq - 1, groups, batch, d), F32), pltpu.VMEM((n_seq - 1, n_groups, 8, lanes), F32),
                pltpu.VMEM((n_seq, lanes, c_groups), F32), pltpu.VMEM((n_seq, lanes, c_groups), F32),
                pltpu.VMEM((batch, groups * d), BF16),
                pltpu.VMEM((chips, batch, blk), F32), pltpu.VMEM((chips, batch, blk), F32),
                pltpu.VMEM((chips, batch, blk), F32), pltpu.VMEM((chips - 1, batch, blk), F32),
                pltpu.VMEM((n_dev, batch, blk), BF16),
                dma((3,)), dma((slots + 1,)), dma((n_groups,)), dma((n_groups,)), dma((2,)), dma((2,)),
                dma((n_groups, n_seq - 1)), dma((n_groups, n_seq - 1)),
                dma((n_groups, n_seq - 1)), dma((n_groups, n_seq - 1)),
                dma((n_c, chips)), dma((n_c, chips)), dma((n_c, chips - 1)), dma((n_c, chips - 1)),
                dma((n_c, chips - 1)), dma((n_c, chips - 1)), dma((n_c, chips)), dma((n_c, chips)),
            ],
            compiler_params=pltpu.CompilerParams(collective_id=0, has_side_effects=True, vmem_limit_bytes=28 * MIB),
        )(positions, tokens, w_query, w_key, w_value, w_out, k_cache.reshape(flat), v_cache.reshape(flat))

        k_out, v_out, y_out, _ = pl.pallas_call(
            functools.partial(write_kernel, (shard, n_groups)), name="write",
            out_shape=(jax.ShapeDtypeStruct(k_cache.shape, BF16), jax.ShapeDtypeStruct(k_cache.shape, BF16),
                       jax.ShapeDtypeStruct(y.shape, BF16), pltpu.VMEM((2, *k_cache.shape), BF16)),
            in_specs=[pl.BlockSpec(memory_space=pltpu.SMEM), vmem, any_spec, vmem],
            out_specs=(any_spec, any_spec, any_spec, vmem),
            scratch_shapes=[dma((2, n_groups)), dma],
            input_output_aliases={3: 3},
            compiler_params=pltpu.CompilerParams(vmem_limit_bytes=4 * MIB),
        )(positions, fresh, y, kv_raw.reshape(2, *k_cache.shape))
        return y_out, k_out, v_out

    return jax.shard_map(
        step,
        mesh=mesh,
        in_specs=(P("rep", None), P(), P(), P(), P(("head", "seq"), None), cache_spec, cache_spec, P("rep")),
        out_specs=(P("rep", None), cache_spec, cache_spec),
        check_vma=False,
    )
```

```python
import functools

import jax
import jax.numpy as jnp
from jax import lax
from jax.experimental import pallas as pl
from jax.experimental.pallas import tpu as pltpu
from jax.sharding import PartitionSpec as P

MESH = pl.DeviceIdType.MESH
BF16 = jnp.bfloat16
F32 = jnp.float32
MIB = 2 ** 20
GB = 8
D = 128
LOG2E = 1.4426950408889634
SCALE2 = (D ** -0.5) * LOG2E
CHUNKS = ((0, 6), (6, 2))


def step_kernel(dims, pos_hbm, x_hbm, wq, wk, wv, wo_hbm, kc, vc, new_s, y_ref, kv_vm,
                pos_ref, x_vm, w_vm, wo_vm, q_s, qt_s, s_s, wt_s, mix_s, st_s, r_mix, r_st, m_t, l_t, o_s,
                p_send, p_recv, y_send, y_recv, y_all,
                in_sem, w_sem, k_sem, v_sem, h_ssem, h_rsem, mix_ssem, mix_rsem, st_ssem, st_rsem,
                p_ssem, p_rsem, y_ssem, y_rsem, a_ssem, a_rsem, f_ssem, f_rsem):
    kv, groups, shard, n_groups, slots, n_seq, n_head, blk = dims
    heads = kv * groups
    rows = shard * kv
    lanes = heads * GB
    head_i, seq_i = lax.axis_index("head"), lax.axis_index("seq")
    x_i, core_i = seq_i // 2, seq_i % 2
    n_x = n_seq // 2
    base = seq_i * shard
    cols = kv * D
    n_q = heads // kv
    partner = {"seq": x_i * 2 + 1 - core_i}
    k_vm, v_vm, nk_s, nv_s = kv_vm.at[0], kv_vm.at[1], new_s.at[0], new_s.at[1]

    barrier = pltpu.get_barrier_semaphore()
    for dh in range(n_head):
        for ds in range(n_seq):
            if dh or ds:
                pl.semaphore_signal(barrier, inc=1, device_id={
                    "head": (head_i + dh) % n_head, "seq": (seq_i + ds) % n_seq}, device_id_type=MESH)

    half_cols = cols // 2
    q_mine = n_q // 2

    def w_copies(c):
        if c < q_mine:
            at = pl.multiple_of(head_i * (heads * D) + (core_i * q_mine + c) * cols, cols)
            return [pltpu.make_async_copy(wq.at[:, pl.ds(at, cols)], w_vm.at[c], w_sem.at[c])]
        at = pl.multiple_of(head_i * cols + core_i * half_cols, half_cols)
        return [pltpu.make_async_copy(src.at[:, pl.ds(at, half_cols)], w_vm.at[c, :, pl.ds(n * half_cols, half_cols)],
                                      w_sem.at[c + n]) for n, src in enumerate((wk, wv))]

    def k_copy(g):
        at = pl.ds(g * GB, GB)
        return pltpu.make_async_copy(kc.at[at], k_vm.at[at], k_sem.at[g])

    def v_copy(g):
        at = pl.ds(g * GB, GB)
        return pltpu.make_async_copy(vc.at[at], v_vm.at[at], v_sem.at[g])

    x_copy = pltpu.make_async_copy(x_hbm, x_vm, in_sem.at[0])
    pos_copy = pltpu.make_async_copy(pos_hbm, pos_ref, in_sem.at[1])
    wo_copy = pltpu.make_async_copy(wo_hbm, wo_vm, in_sem.at[2])
    x_copy.start()
    pos_copy.start()

    ahead = 4
    for c in range(q_mine + 1):
        for copy in w_copies(c):
            copy.start()
    x_copy.wait()
    hq = heads // 2
    q_part = q_s.at[:, pl.ds(pl.multiple_of(core_i * hq, hq), hq)]
    n_part = new_s.at[:, pl.ds(core_i * (kv // 2), kv // 2)]
    q_share = pltpu.make_async_remote_copy(q_part, q_part, h_ssem.at[0], h_rsem.at[0],
                                           device_id=partner, device_id_type=MESH)
    n_share = pltpu.make_async_remote_copy(n_part, n_part, h_ssem.at[1], h_rsem.at[1],
                                           device_id=partner, device_id_type=MESH)
    for c in range(q_mine + 1):
        for copy in w_copies(c):
            copy.wait()
        if c < ahead:
            k_copy(c).start()
            v_copy(c).start()
        r = jnp.dot(x_vm[...], w_vm[c], preferred_element_type=F32)
        r = r.astype(BF16).astype(F32)
        if c < q_mine:
            for i in range(kv):
                q_s[:, core_i * hq + c * kv + i, :] = r[:, i * D:(i + 1) * D]
        else:
            for n in range(2):
                for i in range(kv // 2):
                    new_s[n, core_i * (kv // 2) + i] = r[:, n * half_cols + i * D:n * half_cols + (i + 1) * D]
        if c == q_mine - 1:
            pl.semaphore_wait(barrier, n_head * n_seq - 1)
            q_share.start()
    n_share.start()
    for g in range(q_mine + 1, ahead):
        k_copy(g).start()
        v_copy(g).start()
    q_share.wait()
    n_share.wait()
    pos_copy.wait()

    sub = lax.broadcasted_iota(jnp.int32, (8, lanes), 0)
    lane = lax.broadcasted_iota(jnp.int32, (8, lanes), 1)
    lane_d = lax.broadcasted_iota(jnp.int32, (D, lanes), 1)
    per_tile = 8 // kv
    half = rows // 2

    def rows_of(g):
        return pl.ds(g * GB if isinstance(g, int) else pl.multiple_of(g * GB, GB), GB)

    def scores(g):
        q_t = qt_s[g]
        accs = [None, None]
        for p in range(GB // 2):
            qs = jnp.concatenate([jnp.where(lane_d // heads == 2 * p, q_t, 0.0),
                                  jnp.where(lane_d // heads == 2 * p + 1, q_t, 0.0)], axis=0).astype(BF16)
            for h in range(2):
                at = pl.ds(h * half, half)
                keys = jnp.concatenate([k_vm[g * GB + 2 * p, at, :], k_vm[g * GB + 2 * p + 1, at, :]], axis=1)
                s = jnp.dot(keys, qs, preferred_element_type=F32)
                accs[h] = s if accs[h] is None else accs[h] + s
        for h in range(2):
            s_s[pl.ds(h * (half // 8), half // 8)] = accs[h].reshape(half // 8, 8, lanes)

    def softmax(g):
        pos_row = jnp.zeros((8, lanes), jnp.int32)
        for i in range(GB):
            pos_row = jnp.where(lane // heads == i, pos_ref[g * GB + i] - base, pos_row)
        limit = jnp.where(sub % kv == lane % heads // groups, pos_row - 1 - sub // kv, -1)
        tile_t = lax.broadcasted_iota(jnp.int32, (rows // 8, 8, lanes), 0) * per_tile
        s3 = jnp.where(limit[None] >= tile_t, s_s[...], -jnp.inf)
        m = jnp.max(jnp.max(s3, axis=0), axis=0, keepdims=True)
        m_safe = jnp.where(m > -jnp.inf, m, 0.0)
        w3 = jnp.exp2((s3 - m_safe[None]) * SCALE2)
        total = jnp.sum(jnp.sum(w3, axis=0), axis=0, keepdims=True)
        st_s[g] = jnp.where(sub == 0, m, total)
        wt_s[g % 2] = w3.reshape(rows, lanes).astype(BF16).T

    def values(g):
        for i in range(GB):
            b = g * GB + i
            mix_s[:, b, :] = jnp.dot(wt_s[g % 2, i * heads:(i + 1) * heads, :], v_vm[b], preferred_element_type=F32)

    def mix_copy(g, k):
        to = (seq_i + k) % n_seq
        return pltpu.make_async_remote_copy(
            mix_s.at[pl.ds(to * groups, groups), rows_of(g)], r_mix.at[k - 1, :, rows_of(g)],
            mix_ssem.at[g, k - 1], mix_rsem.at[g, k - 1], device_id={"seq": to}, device_id_type=MESH)

    def st_copy(g, k):
        to = (seq_i + k) % n_seq
        return pltpu.make_async_remote_copy(st_s.at[g], r_st.at[k - 1, g], st_ssem.at[g, k - 1], st_rsem.at[g, k - 1],
                                            device_id={"seq": to}, device_id_type=MESH)

    order = [(dh, dx) for dh in range(n_head - 1, -1, -1) for dx in range(n_x - 1, -1, -1)]
    mine = head_i * n_seq + seq_i

    def block_of(dh, dx, core):
        h, x = (head_i + dh) % n_head, (x_i + dx) % n_x
        return h, x * 2 + core, h * n_seq + x * 2 + core

    def p_copy(c, i):
        at = pl.ds(CHUNKS[c][0] * GB, CHUNKS[c][1] * GB)
        return pltpu.make_async_remote_copy(p_send.at[i, at], p_recv.at[i, at], p_ssem.at[c, i], p_rsem.at[c, i],
                                            device_id=partner, device_id_type=MESH)

    def y_copy(c, dh, dx):
        i = dh * n_x + dx
        at = pl.ds(CHUNKS[c][0] * GB, CHUNKS[c][1] * GB)
        h, s, _ = block_of(dh, dx, core_i)
        return pltpu.make_async_remote_copy(y_send.at[i, at], y_recv.at[i - 1, at], y_ssem.at[c, i - 1],
                                            y_rsem.at[c, i - 1], device_id={"head": h, "seq": s}, device_id_type=MESH)

    def a_copy(c, dh, dx):
        i = dh * n_x + dx
        at = pl.ds(CHUNKS[c][0] * GB, CHUNKS[c][1] * GB)
        h, s, _ = block_of(dh, dx, core_i)
        return pltpu.make_async_remote_copy(y_all.at[mine, at], y_all.at[mine, at], a_ssem.at[c, i - 1],
                                            a_rsem.at[c, i - 1], device_id={"head": h, "seq": s}, device_id_type=MESH)

    def f_copy(c, dh, dx):
        i = dh * n_x + dx
        at = pl.ds(CHUNKS[c][0] * GB, CHUNKS[c][1] * GB)
        _, _, b = block_of(dh, dx, core_i)
        return pltpu.make_async_remote_copy(y_all.at[b, at], y_all.at[b, at], f_ssem.at[c, i], f_rsem.at[c, i],
                                            device_id=partner, device_id_type=MESH)

    def out_products(c):
        g0, n = CHUNKS[c]
        for g in range(g0, g0 + n):
            for k in range(1, n_seq):
                st_copy(g, k).wait()
        for k in range(n_seq):
            src = st_s if k == 0 else r_st.at[k - 1]
            m_t[k, :, 0:n] = jnp.concatenate([src[g, 0:1, :] for g in range(g0, g0 + n)], axis=0).T
            l_t[k, :, 0:n] = jnp.concatenate([src[g, 1:2, :] for g in range(g0, g0 + n)], axis=0).T

        def own(ref, k):
            return jnp.concatenate([ref[k, pl.ds(seq_i * groups + j, GB, stride=heads), 0:n] for j in range(groups)], axis=0)

        ms = [own(m_t, k) for k in range(n_seq)]
        ls = [own(l_t, k) for k in range(n_seq)]
        col = lax.broadcasted_iota(jnp.int32, (GB, n), 1)
        fresh = []
        for j in range(groups):
            s_new = jnp.zeros((GB, n), F32)
            for t in range(n):
                at = pl.ds((g0 + t) * GB, GB)
                dot = jnp.sum(q_s[at, seq_i * groups + j, :] * nk_s[seq_i, at, :], axis=1, keepdims=True)
                s_new = jnp.where(col == t, dot, s_new)
            fresh.append(s_new)
        m_new = jnp.concatenate(fresh, axis=0)
        top = functools.reduce(jnp.maximum, ms + [m_new])
        es = [jnp.exp2((m - top) * SCALE2) for m in ms]
        e_new = jnp.exp2((m_new - top) * SCALE2)
        total = functools.reduce(jnp.add, [l * e for l, e in zip(ls, es)] + [e_new])
        cs = [e / total for e in es]
        c_new = e_new / total
        for g in range(g0, g0 + n):
            for k in range(1, n_seq):
                mix_copy(g, k).wait()
        for j in range(groups):
            tiles = []
            for t in range(n):
                at = pl.ds((g0 + t) * GB, GB)
                o = nv_s[seq_i, at, :] * c_new[j * GB:(j + 1) * GB, t:t + 1]
                for k in range(n_seq):
                    src = mix_s[seq_i * groups + j, at, :] if k == 0 else r_mix[k - 1, j, at, :]
                    o = o + src * cs[k][j * GB:(j + 1) * GB, t:t + 1]
                tiles.append(o)
            o_s[pl.ds(g0 * GB, n * GB), j * D:(j + 1) * D] = jnp.concatenate(tiles, axis=0).astype(BF16)
        at = pl.ds(g0 * GB, n * GB)
        o = o_s[at, :]

        def product(b):
            return jnp.dot(o, wo_vm[:, pl.ds(pl.multiple_of(b * blk, blk), blk)], preferred_element_type=F32)

        for dh, dx in order:
            i = dh * n_x + dx
            p_send[i, at, :] = product(block_of(dh, dx, 1 - core_i)[2])
            p_copy(c, i).start()
        for dh, dx in order:
            y_send[dh * n_x + dx, at, :] = product(block_of(dh, dx, core_i)[2])

    def out_scatter(c):
        at = pl.ds(CHUNKS[c][0] * GB, CHUNKS[c][1] * GB)
        for dh, dx in order:
            i = dh * n_x + dx
            p_copy(c, i).wait_recv()
            y_send[i, at, :] = y_send[i, at, :] + p_recv[i, at, :]
            if i:
                y_copy(c, dh, dx).start()

    def out_gather(c):
        at = pl.ds(CHUNKS[c][0] * GB, CHUNKS[c][1] * GB)
        own = y_send[0, at, :]
        for dh, dx in reversed(order[:-1]):
            y_copy(c, dh, dx).wait_recv()
            own = own + y_recv[dh * n_x + dx - 1, at, :]
        y_all[mine, at, :] = own.astype(BF16)
        for dh, dx in order[:-1]:
            a_copy(c, dh, dx).start()
        f_copy(c, 0, 0).start()

    def out_forward(c):
        for dh, dx in reversed(order[:-1]):
            a_copy(c, dh, dx).wait_recv()
            f_copy(c, dh, dx).start()

    def out_finish(c):
        for dh, dx in order:
            f_copy(c, dh, dx).wait()
            p_copy(c, dh * n_x + dx).wait_send()
            if dh or dx:
                y_copy(c, dh, dx).wait_send()
                a_copy(c, dh, dx).wait_send()

    for g in range(n_groups):
        qt_s[g] = q_s[rows_of(g)].reshape(lanes, D).T
    k_copy(0).wait()
    scores(0)
    softmax(0)
    wo_copy.start()

    def group(g, carry):
        @pl.when(g + ahead < n_groups)
        def _():
            k_copy(g + ahead).start()
            v_copy(g + ahead).start()
        v_copy(g).wait()
        k_copy(g + 1).wait()
        scores(g + 1)
        values(g)
        softmax(g + 1)
        for k in range(1, n_seq):
            st_copy(g, k).start()
            mix_copy(g, k).start()
        return carry

    lax.fori_loop(0, n_groups - 1, group, 0)
    last = n_groups - 1
    v_copy(last).wait()
    values(last)
    for k in range(1, n_seq):
        st_copy(last, k).start()
        mix_copy(last, k).start()
    wo_copy.wait()
    out_products(0)
    out_scatter(0)
    out_products(1)
    out_scatter(1)
    out_gather(0)
    out_forward(0)
    out_gather(1)
    out_forward(1)
    out_finish(0)
    out_finish(1)
    for b in range(n_head * n_seq):
        y_ref[:, b * blk:(b + 1) * blk] = y_all[b]


def write_kernel(dims, pos_ref, new, y_in, kv_in, ko, vo, y_out, kv_vm, o_sem, y_sem):
    shard, n_groups = dims
    del kv_in
    base = lax.axis_index("seq") * shard
    outs = (ko, vo)
    copies = [pltpu.make_async_copy(y_in, y_out, y_sem)]
    copies[0].start()
    for g in range(n_groups):
        for i in range(GB):
            b = g * GB + i
            t = pos_ref[b] - base

            @pl.when(jnp.logical_and(t >= 0, t < shard))
            def _():
                for side in range(2):
                    kv_vm[side, b, t] = new[side, :, b, :].astype(BF16)

        at = pl.ds(g * GB, GB)
        for side in range(2):
            copies.append(pltpu.make_async_copy(kv_vm.at[side, at], outs[side].at[at], o_sem.at[side, g]))
            copies[-1].start()
    for c in copies:
        c.wait()


def solution(mesh):
    n_head, n_seq = mesh.shape["head"], mesh.shape["seq"]
    cache_spec = P("rep", "seq", "head", None)

    def step(tokens, w_query, w_key, w_value, w_out, k_cache, v_cache, positions):
        batch, shard, kv, d = k_cache.shape
        model = tokens.shape[1]
        heads = w_query.shape[1] // d // n_head
        groups = heads // kv
        n_groups = batch // GB
        rows, lanes = shard * kv, heads * GB
        slots = heads // kv // 2 + 1
        n_dev = n_head * n_seq
        blk = w_out.shape[1] // n_dev
        chips = n_head * (n_seq // 2)
        n_c = len(CHUNKS)
        c_groups = max(n for _, n in CHUNKS)
        hbm = pl.BlockSpec(memory_space=pltpu.HBM)
        any_spec = pl.BlockSpec(memory_space=pl.ANY)
        vmem = pl.BlockSpec(memory_space=pltpu.VMEM)
        flat = (batch, rows, d)
        dma = pltpu.SemaphoreType.DMA
        fresh, y, kv_raw = pl.pallas_call(
            functools.partial(step_kernel, (kv, groups, shard, n_groups, slots, n_seq, n_head, blk)),
            name="step",
            out_shape=(pltpu.VMEM((2, kv, batch, d), F32), pltpu.VMEM((batch, w_out.shape[1]), BF16),
                       pltpu.VMEM((2, *flat), BF16)),
            in_specs=[hbm] * 8,
            out_specs=(vmem,) * 3,
            scratch_shapes=[
                pltpu.SMEM((batch,), jnp.int32), pltpu.VMEM((batch, model), BF16),
                pltpu.VMEM((slots, model, kv * d), BF16), pltpu.VMEM(w_out.shape, BF16),
                pltpu.VMEM((batch, heads, d), F32), pltpu.VMEM((n_groups, d, lanes), F32), pltpu.VMEM((rows // 8, 8, lanes), F32),
                pltpu.VMEM((2, lanes, rows), BF16), pltpu.VMEM((heads, batch, d), F32),
                pltpu.VMEM((n_groups, 8, lanes), F32),
                pltpu.VMEM((n_seq - 1, groups, batch, d), F32), pltpu.VMEM((n_seq - 1, n_groups, 8, lanes), F32),
                pltpu.VMEM((n_seq, lanes, c_groups), F32), pltpu.VMEM((n_seq, lanes, c_groups), F32),
                pltpu.VMEM((batch, groups * d), BF16),
                pltpu.VMEM((chips, batch, blk), F32), pltpu.VMEM((chips, batch, blk), F32),
                pltpu.VMEM((chips, batch, blk), F32), pltpu.VMEM((chips - 1, batch, blk), F32),
                pltpu.VMEM((n_dev, batch, blk), BF16),
                dma((3,)), dma((slots + 1,)), dma((n_groups,)), dma((n_groups,)), dma((2,)), dma((2,)),
                dma((n_groups, n_seq - 1)), dma((n_groups, n_seq - 1)),
                dma((n_groups, n_seq - 1)), dma((n_groups, n_seq - 1)),
                dma((n_c, chips)), dma((n_c, chips)), dma((n_c, chips - 1)), dma((n_c, chips - 1)),
                dma((n_c, chips - 1)), dma((n_c, chips - 1)), dma((n_c, chips)), dma((n_c, chips)),
            ],
            compiler_params=pltpu.CompilerParams(collective_id=0, has_side_effects=True, vmem_limit_bytes=28 * MIB),
        )(positions, tokens, w_query, w_key, w_value, w_out, k_cache.reshape(flat), v_cache.reshape(flat))

        k_out, v_out, y_out, _ = pl.pallas_call(
            functools.partial(write_kernel, (shard, n_groups)), name="write",
            out_shape=(jax.ShapeDtypeStruct(k_cache.shape, BF16), jax.ShapeDtypeStruct(k_cache.shape, BF16),
                       jax.ShapeDtypeStruct(y.shape, BF16), pltpu.VMEM((2, *k_cache.shape), BF16)),
            in_specs=[pl.BlockSpec(memory_space=pltpu.SMEM), vmem, any_spec, vmem],
            out_specs=(any_spec, any_spec, any_spec, vmem),
            scratch_shapes=[dma((2, n_groups)), dma],
            input_output_aliases={3: 3},
            compiler_params=pltpu.CompilerParams(vmem_limit_bytes=4 * MIB),
        )(positions, fresh, y, kv_raw.reshape(2, *k_cache.shape))
        return y_out, k_out, v_out

    return jax.shard_map(
        step,
        mesh=mesh,
        in_specs=(P("rep", None), P(), P(), P(), P(("head", "seq"), None), cache_spec, cache_spec, P("rep")),
        out_specs=(P("rep", None), cache_spec, cache_spec),
        check_vma=False,
    )
```
